256 devices in a mesh: slab: 128 (over z, y, x), comp: 2 (over core).
Axes of the slice: x: 4, y: 4, z: 8, core: 2. Of those that a mesh axis runs over, the one named last changes fastest.
Arguments:
- polarization: float32 [6, 128, 128, 128], P('comp', 'slab'), parts along dimension 0, may hold values from -6 to 6
- inverse_polarizability: float32 [128, 128, 128], P('slab'), may hold values from 0.5 to 2
- occupancy: int32 [128, 16, 16], P('slab'), may hold values 0 or 1
- green_fourier: float32 [6, 256, 256, 256], P(None, 'slab'), may hold values from -12 to 12
Outputs:
- first_image: float32 [6, 128, 128, 128], P('comp', 'slab'), parts along dimension 0
- second_image: float32 [6, 128, 128, 128], P('comp', 'slab'), parts along dimension 0
The draws below stay inside these ranges and needn't reach their ends.
There are 2 independent parts, one for each index of `comp`. The reference program is written for one: setup_inputs(seed, part) draws one part's arguments, and reference() takes and returns one part's arrays. A program takes and returns all parts, laid end to end along the dimension named above; an argument that names none is the same for every part. Nothing has to cross between parts.
All inputs are finite; a program needn't handle non-finite values. No bound on the sum of `occupancy` on one device may be relied on, other than what follows from the above.
Results may differ from the reference program's by a relative error of at most 0.0001.
Values sent between devices are 32-bit elements; how exact they have to be, the bound alone decides.
No kernel may reach another device: no remote copies, remote signals or barrier semaphores. Data moves between devices by JAX's collectives and lax.ppermute only.
A program may use at most 64 MiB of HBM per device.

```python
import math
import jax
import jax.numpy as jnp

NY = 128
NZ = 128
BLOCK = 8
MATVECS = 2
NX = 128
LX = 256
LY = 256
LZ = 256


def plant(entries, own_key, smallest, largest):
    index_at = [jax.random.randint(jax.random.fold_in(own_key, axis), (), 0, length) for axis, length in enumerate(entries.shape)]
    main_axis = entries.shape.index(max(entries.shape))
    beside = index_at[:main_axis] + [(index_at[main_axis] + 1) % entries.shape[main_axis]] + index_at[main_axis + 1:]
    return entries.at[tuple(index_at)].set(smallest).at[tuple(beside)].set(largest)


def block_scale(own_key, dims, pieces, least, top_value):
    gain, own = 1.0, jax.random.fold_in(own_key, 6)
    for position, shards_of in pieces:
        heights = jnp.exp(jax.random.uniform(jax.random.fold_in(own, position), (shards_of,), jnp.float32, least / len(pieces), top_value / len(pieces)))
        gain = gain * jnp.repeat(heights, dims[position] // shards_of).reshape([-1 if axis == position else 1 for axis in range(len(dims))])
    return gain


def centred(key, extent, width, reach, shards=(), dtype=jnp.bfloat16):
    factor_of = block_scale(key, extent, shards, -0.22, 0.18) if shards else 1.0
    result = jax.random.normal(key, extent, jnp.float32) * width * factor_of
    return jnp.minimum(jnp.maximum(result, -reach), reach).astype(dtype)


def setup_inputs(seed: int = 0, part: int = 0) -> dict:
    arg_keys = jax.random.split(jax.random.key(seed), 5)
    part_splits = jax.random.split(jax.random.fold_in(arg_keys[4], part), 5)
    polarization = centred(part_splits[0], (3, NX, NY, NZ), 1.0, 6.0, ((1, 128),), jnp.float32)
    inverse_polarizability = jnp.clip(jnp.exp(math.log(2.0) - 1.3862944 * jax.random.uniform(arg_keys[1], (NX, NY, NZ), jnp.float32) ** block_scale(arg_keys[1], (NX, NY, NZ), ((0, 128),), -0.2, 0.2)), 0.5, 2.0)
    occupancy = plant((jax.random.randint(arg_keys[2], (NX, NY // BLOCK, NZ // BLOCK), 0, 4) < 3).astype(jnp.int32), jax.random.fold_in(arg_keys[2], 1), 0, 1)
    green_fourier = centred(arg_keys[3], (6, LZ, LX, LY), 2.0, 12.0, ((1, 128),), jnp.float32)
    return dict(polarization=polarization, inverse_polarizability=inverse_polarizability, occupancy=occupancy, green_fourier=green_fourier)


def expand_mask(occupancy):
    flags = occupancy.astype(jnp.float32)
    first, second, third = flags.shape
    spread = jnp.broadcast_to(flags[:, :, None, :, None], (first, second, BLOCK, third, BLOCK))
    return spread.reshape(first, second * BLOCK, third * BLOCK)


def apply_operator(field, mask, inverse_polarizability, green_ordered):
    masked = field * mask[None]
    padded = jnp.pad(masked, ((0, 0), (0, NX), (0, NY), (0, NZ)))
    spectrum = jnp.fft.fftn(padded, axes=(1, 2, 3))
    combos = ((0, 3, 4), (3, 1, 5), (4, 5, 2))
    results = []
    for row in combos:
        product = green_ordered[row[0]] * spectrum[0] + green_ordered[row[1]] * spectrum[1] + green_ordered[row[2]] * spectrum[2]
        back = jnp.fft.ifftn(product).real[:NX, :NY, :NZ]
        results.append(back.astype(jnp.float32))
    convolved = jnp.stack(results)
    return inverse_polarizability[None] * masked - mask[None] * convolved


def reference(polarization, inverse_polarizability, occupancy, green_fourier):
    mask = expand_mask(occupancy)
    green_ordered = jnp.transpose(green_fourier, (0, 2, 3, 1))
    first_image = apply_operator(polarization, mask, inverse_polarizability, green_ordered)
    current = first_image
    for repeat_index in range(MATVECS - 1):
        current = apply_operator(current, mask, inverse_polarizability, green_ordered)
    return first_image, current
```

```python
import functools

import jax
import jax.numpy as jnp
import numpy as np
from jax import lax
from jax.experimental import pallas as pl
from jax.experimental.pallas import tpu as pltpu
from jax.sharding import PartitionSpec as P

BLOCK = 8
F32 = jnp.float32
BF16 = jnp.bfloat16
PARTS = 3
PLANES = 2
PIECES = PARTS * PLANES * 2


def halves_of(table):
    high = table.astype(jnp.bfloat16)
    low = (table - high.astype(np.float64)).astype(jnp.bfloat16)
    return (high, low)


def angles(count_in, count_out):
    phase = np.outer(np.arange(count_in), np.arange(count_out)) % count_out
    return 2.0 * np.pi * phase / count_out


def plane_tables(cells):
    angle = angles(cells, 2 * cells)
    cosine, sine = np.cos(angle), np.sin(angle)
    table = np.block([[cosine, -sine], [sine, cosine]])
    return halves_of(table) + halves_of(np.ascontiguousarray(table.T))


def z_tables(cells, devices):
    angle = angles(cells, 2 * cells)
    per_owner = 2 * cells // devices
    both = np.stack([np.cos(angle).T, -np.sin(angle).T])
    both = both.reshape(2, devices, per_owner, cells).transpose(2, 0, 1, 3)
    table = both.reshape(4 * cells, cells)
    return halves_of(table) + halves_of(np.ascontiguousarray(table.T) / float((2 * cells) ** 3))


def split(value):
    high = value.astype(BF16)
    return (high, (value - high.astype(F32)).astype(BF16))


def dot3(left, right, dims=((1,), (0,))):
    def one(a, b):
        return lax.dot_general(a, b, (dims, ((), ())), preferred_element_type=F32)

    return one(left[0], right[0]) + one(left[1], right[0]) + one(left[0], right[1])


def mask_of(occupancy, cells):
    blocks = occupancy.shape[-1]
    row = lax.broadcasted_iota(jnp.int32, (cells, blocks), 0)
    col = lax.broadcasted_iota(jnp.int32, (cells, blocks), 1)
    expand = jnp.where(row // BLOCK == col, 1.0, 0.0).astype(F32)
    flags = occupancy.astype(F32)
    rows = jnp.dot(expand, flags, preferred_element_type=F32)
    return lax.dot_general(rows, expand, (((1,), (1,)), ((), ())), preferred_element_type=F32)


def put_pieces(out_ref, part, spread, devices):
    for plane in range(PLANES):
        for kind in range(2):
            piece = (part * PLANES + plane) * 2 + kind
            start = (plane * 2 + kind) * devices
            out_ref[pl.ds(piece, devices, stride=PIECES), :] = spread[start : start + devices]


def forward_z_kernel(field_ref, occupancy_ref, high_ref, low_ref, out_ref):
    cells = field_ref.shape[-1]
    devices = out_ref.shape[0] // PIECES
    mask = mask_of(occupancy_ref[0], cells)
    table = (high_ref[...], low_ref[...])
    for part in range(PARTS):
        masked = split(field_ref[part, 0] * mask)
        spread = dot3(table, masked, ((1,), (1,)))
        put_pieces(out_ref, part, spread, devices)


def image_of(part, data_ref, field_ref, inverse_ref, mask, table, devices):
    stack = [
        data_ref[pl.ds((part * PLANES + plane) * 2 + kind, devices, stride=PIECES), :]
        for plane in range(PLANES)
        for kind in range(2)
    ]
    convolved = dot3(table, split(jnp.concatenate(stack, axis=0))).T
    masked = field_ref[part, 0] * mask
    return inverse_ref[0] * masked - mask * convolved


def middle_z_kernel(
    data_ref, field_ref, inverse_ref, occupancy_ref, high_ref, low_ref, back_high_ref, back_low_ref, image_ref, out_ref
):
    cells = field_ref.shape[-1]
    devices = out_ref.shape[0] // PIECES
    mask = mask_of(occupancy_ref[0], cells)
    table = (high_ref[...], low_ref[...])
    back = (back_high_ref[...], back_low_ref[...])
    for part in range(PARTS):
        image = image_of(part, data_ref, field_ref, inverse_ref, mask, back, devices)
        image_ref[part, 0] = image
        spread = dot3(table, split(image * mask), ((1,), (1,)))
        put_pieces(out_ref, part, spread, devices)


def last_z_kernel(data_ref, field_ref, inverse_ref, occupancy_ref, back_high_ref, back_low_ref, image_ref):
    cells = field_ref.shape[-1]
    devices = data_ref.shape[0] // PIECES
    mask = mask_of(occupancy_ref[0], cells)
    back = (back_high_ref[...], back_low_ref[...])
    for part in range(PARTS):
        image_ref[part, 0] = image_of(part, data_ref, field_ref, inverse_ref, mask, back, devices)


def plane_kernel(data_ref, green_ref, high_ref, low_ref, t_high_ref, t_low_ref, out_ref, spectrum_ref):
    devices = data_ref.shape[0] // PIECES
    length = green_ref.shape[-1]
    combos = ((0, 3, 4), (3, 1, 5), (4, 5, 2))
    table = (high_ref[...], low_ref[...])
    table_t = (t_high_ref[...], t_low_ref[...])
    for plane in range(PLANES):

        def piece_of(part, kind):
            return pl.ds((part * PLANES + plane) * 2 + kind, devices, stride=PIECES)

        for part in range(PARTS):
            rows = jnp.concatenate([data_ref[piece_of(part, 0), :], data_ref[piece_of(part, 1), :]], axis=1)
            along_y = dot3(split(rows), table)
            stacked = jnp.concatenate([along_y[:, :length], along_y[:, length:]], axis=0)
            spectrum_ref[part] = dot3(table_t, split(stacked))
        for part in range(PARTS):
            row = combos[part]
            first, second, third = green_ref[row[0], plane], green_ref[row[1], plane], green_ref[row[2], plane]

            def product(kind):
                where = slice(kind * length, (kind + 1) * length)
                return (
                    first * spectrum_ref[0, where] + second * spectrum_ref[1, where] + third * spectrum_ref[2, where]
                )

            field = jnp.concatenate([product(0), product(1)], axis=0)
            along_x = dot3(table, split(field))
            rows = jnp.concatenate([along_x[:devices], along_x[devices:]], axis=1)
            back = dot3(split(rows), table_t)
            out_ref[piece_of(part, 0), :] = back[:, :devices]
            out_ref[piece_of(part, 1), :] = back[:, devices:]


VMEM = pl.BlockSpec(memory_space=pltpu.VMEM)


def call(kernel, outs, args, flops, scratch=()):
    single = not isinstance(outs, tuple)
    moved = sum(a.size * a.dtype.itemsize for a in args)
    return pl.pallas_call(
        kernel,
        out_shape=outs,
        in_specs=[VMEM] * len(args),
        out_specs=VMEM if single else (VMEM,) * len(outs),
        scratch_shapes=list(scratch),
        cost_estimate=pl.CostEstimate(flops=flops, bytes_accessed=moved, transcendentals=0),
        compiler_params=pltpu.CompilerParams(vmem_limit_bytes=48 * 1024 * 1024),
    )(*args)


def exchange(data, devices):
    rows = data.shape[0] // devices
    flat = data.reshape(devices, 1, rows * data.shape[1])
    moved = lax.all_to_all(flat, "slab", split_axis=0, concat_axis=0, tiled=True)
    return moved.reshape(data.shape)


def per_device(devices, polarization, inverse_polarizability, occupancy, green_fourier):
    cells = polarization.shape[-1]
    length = green_fourier.shape[-1]
    z_high, z_low, back_high, back_low = (jnp.asarray(t) for t in z_tables(cells, devices))
    planes = tuple(jnp.asarray(t) for t in plane_tables(cells))
    sent = jax.ShapeDtypeStruct((devices * PIECES, cells), F32)
    image = jax.ShapeDtypeStruct(polarization.shape, F32)
    z_flops = 3 * 2 * PARTS * cells * cells * 2 * length
    plane_flops = 3 * 2 * PARTS * PLANES * (4 * cells * cells * length + 4 * cells * length * length) * 2

    def planes_of(data):
        scratch = (pltpu.VMEM((PARTS, 2 * length, length), F32),)
        return call(plane_kernel, sent, (data, green_fourier) + planes, plane_flops, scratch)

    data = call(forward_z_kernel, sent, (polarization, occupancy, z_high, z_low), z_flops)
    data = exchange(planes_of(exchange(data, devices)), devices)
    first_image, data = call(
        middle_z_kernel,
        (image, sent),
        (data, polarization, inverse_polarizability, occupancy, z_high, z_low, back_high, back_low),
        2 * z_flops,
    )
    data = exchange(planes_of(exchange(data, devices)), devices)
    second_image = call(
        last_z_kernel,
        image,
        (data, first_image, inverse_polarizability, occupancy, back_high, back_low),
        z_flops,
    )
    return (first_image, second_image)


def solution(mesh):
    return jax.shard_map(
        functools.partial(per_device, mesh.shape["slab"]),
        mesh=mesh,
        in_specs=(
            P("comp", "slab", None, None),
            P("slab", None, None),
            P("slab", None, None),
            P(None, "slab", None, None),
        ),
        out_specs=(P("comp", "slab", None, None), P("comp", "slab", None, None)),
        check_vma=False,
    )
```

```python
import functools

import jax
import jax.numpy as jnp
import numpy as np
from jax import lax
from jax.experimental import pallas as pl
from jax.experimental.pallas import tpu as pltpu
from jax.sharding import PartitionSpec as P


BLOCK = 8
F32 = jnp.float32
BF16 = jnp.bfloat16
PARTS = 3
PIECES = PARTS * 2
COMBOS = ((0, 3, 4), (3, 1, 5), (4, 5, 2))


def halves_of(table):
    high = table.astype(jnp.bfloat16)
    low = (table - high.astype(np.float64)).astype(jnp.bfloat16)
    return (high, low)


def plane_tables(cells):
    phase = np.outer(np.arange(cells), np.arange(2 * cells)) % (2 * cells)
    angle = np.pi * phase / cells
    cosine, sine = np.cos(angle), np.sin(angle)
    table = np.block([[cosine, -sine], [sine, cosine]])
    return halves_of(table) + halves_of(np.ascontiguousarray(table.T))


def kept_plane(owner, devices):
    return 0 if owner < devices // 2 else 1


def pair_of(owner, devices):
    if owner < devices // 2:
        return devices - 1 - owner
    return devices - owner if owner > devices // 2 else 0


def z_tables(cells, devices):
    wave = np.array([2 * d + kept_plane(d, devices) for d in range(devices)])
    angle = np.pi * (np.outer(wave, np.arange(cells)) % (2 * cells)) / cells
    both = np.stack([np.cos(angle), -np.sin(angle)])
    both[1, 0] = np.cos(np.pi * np.arange(cells))
    table = both.reshape(2 * devices, cells)
    return halves_of(table) + halves_of(np.ascontiguousarray(table.T) / float((2 * cells) ** 3))


def split(value):
    high = value.astype(BF16)
    return (high, (value - high.astype(F32)).astype(BF16))


def dot(left, right, dims=((1,), (0,))):
    return lax.dot_general(left, right, (dims, ((), ())), preferred_element_type=F32)


def dot3(left, right, dims=((1,), (0,))):
    return dot(left[0], right[0], dims) + dot(left[1], right[0], dims) + dot(left[0], right[1], dims)


def mask_of(occupancy, cells):
    blocks = occupancy.shape[-1]
    row = lax.broadcasted_iota(jnp.int32, (cells, blocks), 0)
    col = lax.broadcasted_iota(jnp.int32, (cells, blocks), 1)
    expand = jnp.where(row // BLOCK == col, 1.0, 0.0).astype(F32)
    return dot(dot(expand, occupancy.astype(F32)), expand, ((1,), (1,)))


def put_pieces(out_ref, part, spread, devices):
    for kind in range(2):
        out_ref[pl.ds(part * 2 + kind, devices, stride=PIECES), :] = spread[kind * devices : (kind + 1) * devices]


def get_pieces(data_ref, part, devices, axis):
    pieces = [data_ref[pl.ds(part * 2 + kind, devices, stride=PIECES), :] for kind in range(2)]
    return jnp.concatenate(pieces, axis=axis)


def copies_of(pairs, semaphores):
    copies = [pltpu.make_async_copy(src, dst, semaphores.at[i]) for i, (src, dst) in enumerate(pairs)]
    for copy in copies:
        copy.start()
    return copies


def forward_z_kernel(*refs):
    sources, out_ref, (field_ref, occupancy_ref, high_ref, low_ref), semaphores = refs[:4], refs[4], refs[5:9], refs[9]
    for copy in copies_of(list(zip(sources, refs[5:9])), semaphores):
        copy.wait()
    cells = field_ref.shape[-1]
    devices = out_ref.shape[0] // PIECES
    mask = mask_of(occupancy_ref[0], cells)
    table = (high_ref[...], low_ref[...])
    for part in range(PARTS):
        spread = dot3(table, split(field_ref[part, 0] * mask), ((1,), (1,)))
        put_pieces(out_ref, part, spread, devices)


def image_of(part, data_ref, field_ref, inverse_ref, mask, table, devices):
    convolved = dot3(table, split(get_pieces(data_ref, part, devices, 0))).T
    masked = field_ref[part, 0] * mask
    return inverse_ref[0] * masked - mask * convolved


def middle_z_kernel(
    data_ref, field_ref, inverse_ref, occupancy_ref, high_ref, low_ref, back_high_ref, back_low_ref, image_ref, out_ref
):
    cells = field_ref.shape[-1]
    devices = out_ref.shape[0] // PIECES
    mask = mask_of(occupancy_ref[0], cells)
    table = (high_ref[...], low_ref[...])
    back = (back_high_ref[...], back_low_ref[...])
    for part in range(PARTS):
        image = image_of(part, data_ref, field_ref, inverse_ref, mask, back, devices)
        image_ref[part, 0] = image
        spread = dot3(table, split(image * mask), ((1,), (1,)))
        put_pieces(out_ref, part, spread, devices)


def last_z_kernel(data_ref, field_ref, inverse_ref, occupancy_ref, back_high_ref, back_low_ref, image_ref):
    cells = field_ref.shape[-1]
    devices = data_ref.shape[0] // PIECES
    mask = mask_of(occupancy_ref[0], cells)
    back = (back_high_ref[...], back_low_ref[...])
    for part in range(PARTS):
        image_ref[part, 0] = image_of(part, data_ref, field_ref, inverse_ref, mask, back, devices)


def pair_kernel(
    green_ref, mine_hbm, other_hbm, sum_ref, difference_ref, own_ref, mine_ref, other_ref, semaphores, *, devices
):
    length = own_ref.shape[-1]
    slab = lax.axis_index("slab")
    first = slab == 0
    kept = jnp.where(slab >= devices // 2, 1, 0)
    pairs = [(green_ref.at[:, kept], own_ref), (mine_hbm, mine_ref), (other_hbm, other_ref)]
    for copy in copies_of(pairs, semaphores):
        copy.wait()
    core = lax.axis_index("comp")
    row = lax.broadcasted_iota(jnp.int32, (length, length), 0)
    col = lax.broadcasted_iota(jnp.int32, (length, length), 1)
    flip = jnp.where((row + col == length) | (row + col == 0), 1.0, 0.0).astype(BF16)

    def flipped(value):
        high, low = split(value)

        def one(half):
            return dot(flip, dot(half, flip).astype(BF16))

        return one(high) + one(low)

    for here in range(PARTS):
        for received, start in ((mine_ref, core * PARTS), (other_ref, (1 - core) * PARTS)):
            entry = start + here
            own = own_ref[entry]
            pair = received[here, 0]
            pair_flipped = flipped(pair)

            @pl.when(jnp.logical_not(first))
            def _():
                sum_ref[entry] = own + pair_flipped

            @pl.when(first)
            def _():
                own_both = own + flipped(own)
                pair_both = pair + pair_flipped
                sum_ref[entry] = 0.25 * (own_both + pair_both)
                difference_ref[entry] = 0.25 * (own_both - pair_both)


def plane_kernel(data_ref, *refs):
    sources, out_ref, buffers = refs[:6], refs[6], refs[7:13]
    spectrum_ref, field_ref, semaphores = refs[13:]
    tables, (sum_ref, difference_ref) = buffers[:4], buffers[4:]
    copies = copies_of(list(zip(sources[:5], buffers[:5])), semaphores)
    devices = data_ref.shape[0] // PIECES
    length = sum_ref.shape[-1]
    for copy in copies[:4]:
        copy.wait()
    table = (tables[0][...], tables[1][...])
    table_t = (tables[2][...], tables[3][...])

    def transform(sign):
        for part in range(PARTS):
            rows = get_pieces(data_ref, part, devices, 1)
            if sign < 0:
                rows = jnp.concatenate([rows[:, :devices], -rows[:, devices:]], axis=1)
            along_y = dot3(split(rows), table)
            stacked = jnp.concatenate([along_y[:, :length], along_y[:, length:]], axis=0)
            spectrum_ref[part] = dot3(table_t, split(stacked))

    def product(green_ref, part, kind):
        where = slice(kind * length, (kind + 1) * length)
        first, second, third = COMBOS[part]
        return (
            green_ref[first] * spectrum_ref[0, where]
            + green_ref[second] * spectrum_ref[1, where]
            + green_ref[third] * spectrum_ref[2, where]
        )

    transform(1)
    copies[4].wait()
    for part in range(PARTS):
        for kind in range(2):
            field_ref[part, kind * length : (kind + 1) * length] = product(sum_ref, part, kind)

    @pl.when(lax.axis_index("slab") == 0)
    def _():
        copy = pltpu.make_async_copy(sources[5], difference_ref, semaphores.at[5])
        copy.start()
        transform(-1)
        copy.wait()
        for part in range(PARTS):
            for kind in range(2):
                field_ref[part, kind * length : (kind + 1) * length] += product(difference_ref, part, kind)

    for part in range(PARTS):
        along_x = dot3(table, split(field_ref[part]))
        rows = jnp.concatenate([along_x[:devices], along_x[devices:]], axis=1)
        back = dot3(split(rows), table_t)
        for kind in range(2):
            out_ref[pl.ds(part * 2 + kind, devices, stride=PIECES), :] = back[:, kind * devices : (kind + 1) * devices]


VMEM = pl.BlockSpec(memory_space=pltpu.VMEM)
ANY = pl.BlockSpec(memory_space=pltpu.HBM)


def buffers_for(arrays):
    return [pltpu.VMEM(a.shape, a.dtype) for a in arrays]


def call(kernel, outs, args, flops, scratch=(), mebibytes=8, specs=None):
    single = not isinstance(outs, tuple)
    moved = sum(a.size * a.dtype.itemsize for a in args)
    return pl.pallas_call(
        kernel,
        out_shape=outs,
        in_specs=specs or [VMEM] * len(args),
        out_specs=VMEM if single else (VMEM,) * len(outs),
        scratch_shapes=list(scratch),
        cost_estimate=pl.CostEstimate(flops=flops, bytes_accessed=moved, transcendentals=0),
        compiler_params=pltpu.CompilerParams(vmem_limit_bytes=mebibytes * 1024 * 1024),
    )(*args)


def exchange(data, devices):
    rows = data.shape[0] // devices
    flat = data.reshape(devices, 1, rows * data.shape[1])
    moved = lax.all_to_all(flat, "slab", split_axis=0, concat_axis=0, tiled=True)
    return moved.reshape(data.shape)


def per_device(devices, polarization, inverse_polarizability, occupancy, green_fourier):
    cells = polarization.shape[-1]
    length = green_fourier.shape[-1]
    slab, core = lax.axis_index("slab"), lax.axis_index("comp")
    kept = (slab >= devices // 2).astype(jnp.int32)
    given = lax.dynamic_slice(green_fourier, (core * PARTS, 1 - kept, 0, 0), (PARTS, 1, length, length))
    mine = lax.ppermute(given, "slab", [(d, pair_of(d, devices)) for d in range(devices)])
    other = lax.ppermute(mine, "comp", [(0, 1), (1, 0)])

    z_high, z_low, back_high, back_low = (jnp.asarray(t) for t in z_tables(cells, devices))
    planes = tuple(jnp.asarray(t) for t in plane_tables(cells))
    sent = jax.ShapeDtypeStruct((devices * PIECES, cells), F32)
    image = jax.ShapeDtypeStruct(polarization.shape, F32)
    green = jax.ShapeDtypeStruct((2 * PARTS, length, length), F32)
    z_flops = 3 * 2 * PARTS * cells * cells * length
    plane_flops = 3 * 2 * PARTS * (4 * cells * cells * length + 4 * cells * length * length) * 2

    args = (polarization, occupancy, z_high, z_low)
    scratch = buffers_for(args) + [pltpu.SemaphoreType.DMA((4,))]
    data = call(forward_z_kernel, sent, args, z_flops, scratch, specs=[ANY] * 4)
    data = exchange(data, devices)
    args = (green_fourier, mine, other)
    scratch = [pltpu.VMEM(green.shape, F32)] + buffers_for(args[1:]) + [pltpu.SemaphoreType.DMA((3,))]
    pairing = functools.partial(pair_kernel, devices=devices)
    greens = call(pairing, (green, green), args, 4 * 2 * 2 * PARTS * length**3, scratch, 16, [ANY] * 3)

    def planes_of(data):
        args = planes + tuple(greens)
        scratch = buffers_for(args) + [pltpu.VMEM((PARTS, 2 * length, length), F32)] * 2
        scratch = scratch + [pltpu.SemaphoreType.DMA((6,))]
        return call(plane_kernel, sent, (data,) + args, plane_flops, scratch, 24, [VMEM] + [ANY] * 6)

    data = exchange(planes_of(data), devices)
    first_image, data = call(
        middle_z_kernel,
        (image, sent),
        (data, polarization, inverse_polarizability, occupancy, z_high, z_low, back_high, back_low),
        2 * z_flops,
    )
    data = exchange(planes_of(exchange(data, devices)), devices)
    second_image = call(
        last_z_kernel,
        image,
        (data, first_image, inverse_polarizability, occupancy, back_high, back_low),
        z_flops,
    )
    return (first_image, second_image)


def solution(mesh):
    def body(*args):
        return per_device(mesh.shape["slab"], *args)

    return jax.shard_map(
        body,
        mesh=mesh,
        in_specs=(
            P("comp", "slab", None, None),
            P("slab", None, None),
            P("slab", None, None),
            P(None, "slab", None, None),
        ),
        out_specs=(P("comp", "slab", None, None), P("comp", "slab", None, None)),
        check_vma=False,
    )
```

```python
import functools

import jax
import jax.numpy as jnp
import numpy as np
from jax import lax
from jax.experimental import pallas as pl
from jax.experimental.pallas import tpu as pltpu
from jax.sharding import PartitionSpec as P

BLOCK = 8
LANES = 128
BEHIND = 14000
F32 = jnp.float32
BF16 = jnp.bfloat16
PARTS = 3
PLANES = 2
PIECES = PARTS * PLANES * 2


def halves_of(table):
    high = table.astype(jnp.bfloat16)
    low = (table - high.astype(np.float64)).astype(jnp.bfloat16)
    return (high, low)


def angles(count_in, count_out):
    phase = np.outer(np.arange(count_in), np.arange(count_out)) % count_out
    return 2.0 * np.pi * phase / count_out


def tables_of(cells, devices):
    angle = angles(cells, 2 * cells)
    cosine, sine = np.cos(angle), np.sin(angle)
    plane = np.block([[cosine, -sine], [sine, cosine]])
    both = np.stack([cosine.T, -sine.T]).reshape(2, devices, 2 * cells // devices, cells)
    along_z = both.transpose(2, 0, 1, 3).reshape(4 * cells, cells)
    return (along_z, along_z.T / float((2 * cells) ** 3), plane, plane.T)


def packed_tables(cells, devices):
    blocks, where, row = [], [], 0
    for table in tables_of(cells, devices):
        rows, columns = table.shape
        for half in halves_of(table):
            where.append((row, rows, columns))
            for start in range(0, columns, LANES):
                blocks.append(half[:, start : start + LANES])
                row += rows
    return np.concatenate(blocks, axis=0), where


def table_from(tables_ref, entry):
    def half(row, rows, columns):
        return jnp.concatenate(
            [tables_ref[row + i * rows : row + (i + 1) * rows] for i in range(columns // LANES)], axis=1
        )

    return tuple(half(*one) for one in entry)


def split(value):
    high = value.astype(BF16)
    return (high, (value - high.astype(F32)).astype(BF16))


def dot3(left, right, dims=((1,), (0,))):
    def one(a, b):
        return lax.dot_general(a, b, (dims, ((), ())), preferred_element_type=F32)

    return one(left[0], right[0]) + one(left[1], right[0]) + one(left[0], right[1])


def mask_of(occupancy, cells):
    blocks = occupancy.shape[-1]
    row = lax.broadcasted_iota(jnp.int32, (cells, blocks), 0)
    col = lax.broadcasted_iota(jnp.int32, (cells, blocks), 1)
    expand = jnp.where(row // BLOCK == col, 1.0, 0.0).astype(F32)
    flags = occupancy.astype(F32)
    rows = jnp.dot(expand, flags, preferred_element_type=F32)
    return lax.dot_general(rows, expand, (((1,), (1,)), ((), ())), preferred_element_type=F32)


def put_pieces(out_ref, part, spread, devices):
    for plane in range(PLANES):
        for kind in range(2):
            piece = (part * PLANES + plane) * 2 + kind
            start = (plane * 2 + kind) * devices
            out_ref[pl.ds(piece, devices, stride=PIECES), :] = spread[start : start + devices]


def forward_z_kernel(field_ref, occupancy_ref, tables_ref, green_ref, out_ref, *, where):
    cells = field_ref.shape[-1]
    devices = out_ref.shape[0] // PIECES
    mask = mask_of(occupancy_ref[0], cells)
    table = table_from(tables_ref, where[0:2])
    for part in range(PARTS):
        masked = split(field_ref[part, 0] * mask)
        spread = dot3(table, masked, ((1,), (1,)))
        put_pieces(out_ref, part, spread, devices)

    @pl.when(lax.axis_index("comp") == 1)
    def _():
        pl.delay(BEHIND)


def image_of(part, data_ref, field_ref, inverse_ref, mask, table, devices):
    stack = [
        data_ref[pl.ds((part * PLANES + plane) * 2 + kind, devices, stride=PIECES), :]
        for plane in range(PLANES)
        for kind in range(2)
    ]
    convolved = dot3(table, split(jnp.concatenate(stack, axis=0))).T
    masked = field_ref[part, 0] * mask
    return inverse_ref[0] * masked - mask * convolved


def middle_z_kernel(data_ref, field_ref, inverse_ref, occupancy_ref, tables_ref, image_ref, out_ref, *, where):
    cells = field_ref.shape[-1]
    devices = out_ref.shape[0] // PIECES
    mask = mask_of(occupancy_ref[0], cells)
    table = table_from(tables_ref, where[0:2])
    back = table_from(tables_ref, where[2:4])
    for part in range(PARTS):
        image = image_of(part, data_ref, field_ref, inverse_ref, mask, back, devices)
        image_ref[part, 0] = image
        spread = dot3(table, split(image * mask), ((1,), (1,)))
        put_pieces(out_ref, part, spread, devices)


def last_z_kernel(data_ref, field_ref, inverse_ref, occupancy_ref, tables_ref, image_ref, *, where):
    cells = field_ref.shape[-1]
    devices = data_ref.shape[0] // PIECES
    mask = mask_of(occupancy_ref[0], cells)
    back = table_from(tables_ref, where[2:4])
    for part in range(PARTS):
        image_ref[part, 0] = image_of(part, data_ref, field_ref, inverse_ref, mask, back, devices)


def plane_kernel(data_ref, green_ref, tables_ref, out_ref, spectrum_ref, *, where):
    devices = data_ref.shape[0] // PIECES
    length = green_ref.shape[-1]
    combos = ((0, 3, 4), (3, 1, 5), (4, 5, 2))
    table = table_from(tables_ref, where[4:6])
    table_t = table_from(tables_ref, where[6:8])
    for plane in range(PLANES):

        def piece_of(part, kind):
            return pl.ds((part * PLANES + plane) * 2 + kind, devices, stride=PIECES)

        for part in range(PARTS):
            rows = jnp.concatenate([data_ref[piece_of(part, 0), :], data_ref[piece_of(part, 1), :]], axis=1)
            along_y = dot3(split(rows), table)
            stacked = jnp.concatenate([along_y[:, :length], along_y[:, length:]], axis=0)
            spectrum_ref[part] = dot3(table_t, split(stacked))
        for part in range(PARTS):
            row = combos[part]
            first, second, third = green_ref[row[0], plane], green_ref[row[1], plane], green_ref[row[2], plane]

            def product(kind):
                where = slice(kind * length, (kind + 1) * length)
                return (
                    first * spectrum_ref[0, where] + second * spectrum_ref[1, where] + third * spectrum_ref[2, where]
                )

            field = jnp.concatenate([product(0), product(1)], axis=0)
            along_x = dot3(table, split(field))
            rows = jnp.concatenate([along_x[:devices], along_x[devices:]], axis=1)
            back = dot3(split(rows), table_t)
            out_ref[piece_of(part, 0), :] = back[:, :devices]
            out_ref[piece_of(part, 1), :] = back[:, devices:]


VMEM = pl.BlockSpec(memory_space=pltpu.VMEM)


def call(kernel, outs, args, flops, scratch=(), mebibytes=12):
    single = not isinstance(outs, tuple)
    moved = sum(a.size * a.dtype.itemsize for a in args)
    return pl.pallas_call(
        kernel,
        out_shape=outs,
        in_specs=[VMEM] * len(args),
        out_specs=VMEM if single else (VMEM,) * len(outs),
        scratch_shapes=list(scratch),
        cost_estimate=pl.CostEstimate(flops=flops, bytes_accessed=moved, transcendentals=0),
        compiler_params=pltpu.CompilerParams(vmem_limit_bytes=mebibytes * 1024 * 1024),
    )(*args)


def exchange(data, devices):
    rows = data.shape[0] // devices
    flat = data.reshape(devices, 1, rows * data.shape[1])
    moved = lax.all_to_all(flat, "slab", split_axis=0, concat_axis=0, tiled=True)
    return moved.reshape(data.shape)


def per_device(devices, polarization, inverse_polarizability, occupancy, green_fourier):
    cells = polarization.shape[-1]
    length = green_fourier.shape[-1]
    packed, where = packed_tables(cells, devices)
    tables = jnp.asarray(packed)
    sent = jax.ShapeDtypeStruct((devices * PIECES, cells), F32)
    image = jax.ShapeDtypeStruct(polarization.shape, F32)
    z_flops = 3 * 2 * PARTS * cells * cells * 2 * length
    plane_flops = 3 * 2 * PARTS * PLANES * (4 * cells * cells * length + 4 * cells * length * length) * 2

    def using(kernel):
        return functools.partial(kernel, where=where)

    def planes_of(data):
        scratch = (pltpu.VMEM((PARTS, 2 * length, length), F32),)
        return call(using(plane_kernel), sent, (data, green_fourier, tables), plane_flops, scratch)

    data = call(using(forward_z_kernel), sent, (polarization, occupancy, tables, green_fourier), z_flops)
    data = exchange(planes_of(exchange(data, devices)), devices)
    first_image, data = call(
        using(middle_z_kernel),
        (image, sent),
        (data, polarization, inverse_polarizability, occupancy, tables),
        2 * z_flops,
    )
    data = exchange(planes_of(exchange(data, devices)), devices)
    second_image = call(
        using(last_z_kernel), image, (data, first_image, inverse_polarizability, occupancy, tables), z_flops
    )
    return (first_image, second_image)


def solution(mesh):
    return jax.shard_map(
        functools.partial(per_device, mesh.shape["slab"]),
        mesh=mesh,
        in_specs=(
            P("comp", "slab", None, None),
            P("slab", None, None),
            P("slab", None, None),
            P(None, "slab", None, None),
        ),
        out_specs=(P("comp", "slab", None, None), P("comp", "slab", None, None)),
        check_vma=False,
    )
```

```python
import functools

import jax
import jax.numpy as jnp
import numpy as np
from jax import lax
from jax.experimental import pallas as pl
from jax.experimental.pallas import tpu as pltpu
from jax.sharding import PartitionSpec as P

BLOCK = 8
LANES = 128
BEHIND = 14000
F32 = jnp.float32
BF16 = jnp.bfloat16
PARTS = 3
PLANES = 2
PIECES = PARTS * PLANES * 2


def halves_of(table):
    high = table.astype(jnp.bfloat16)
    low = (table - high.astype(np.float64)).astype(jnp.bfloat16)
    return (high, low)


def angles(count_in, count_out):
    phase = np.outer(np.arange(count_in), np.arange(count_out)) % count_out
    return 2.0 * np.pi * phase / count_out


def tables_of(cells, devices):
    angle = angles(cells, 2 * cells)
    cosine, sine = np.cos(angle), np.sin(angle)
    plane = np.block([[cosine, -sine], [sine, cosine]])
    both = np.stack([cosine.T, -sine.T]).reshape(2, devices, 2 * cells // devices, cells)
    along_z = both.transpose(2, 0, 1, 3).reshape(4 * cells, cells)
    return (along_z, along_z.T / float((2 * cells) ** 3), plane, plane.T)


def packed_tables(cells, devices):
    blocks, where, row = [], [], 0
    for table in tables_of(cells, devices):
        rows, columns = table.shape
        for half in halves_of(table):
            where.append((row, rows, columns))
            for start in range(0, columns, LANES):
                blocks.append(half[:, start : start + LANES])
                row += rows
    return np.concatenate(blocks, axis=0), where


def table_from(tables_ref, entry):
    def half(row, rows, columns):
        return jnp.concatenate(
            [tables_ref[row + i * rows : row + (i + 1) * rows] for i in range(columns // LANES)], axis=1
        )

    return tuple(half(*one) for one in entry)


def split(value):
    high = value.astype(BF16)
    return (high, (value - high.astype(F32)).astype(BF16))


def dot3(left, right, dims=((1,), (0,))):
    def one(a, b):
        return lax.dot_general(a, b, (dims, ((), ())), preferred_element_type=F32)

    rows = left[0].shape[0]
    both = one(jnp.concatenate(left, axis=0), right[0])
    return both[:rows] + both[rows:] + one(left[0], right[1])


def mask_of(occupancy, cells):
    blocks = occupancy.shape[-1]
    row = lax.broadcasted_iota(jnp.int32, (cells, blocks), 0)
    col = lax.broadcasted_iota(jnp.int32, (cells, blocks), 1)
    expand = jnp.where(row // BLOCK == col, 1.0, 0.0).astype(F32)
    flags = occupancy.astype(F32)
    rows = jnp.dot(expand, flags, preferred_element_type=F32)
    return lax.dot_general(rows, expand, (((1,), (1,)), ((), ())), preferred_element_type=F32)


def put_pieces(out_ref, part, spread, devices):
    for plane in range(PLANES):
        for kind in range(2):
            piece = (part * PLANES + plane) * 2 + kind
            start = (plane * 2 + kind) * devices
            out_ref[pl.ds(piece, devices, stride=PIECES), :] = spread[start : start + devices]


def forward_z_kernel(field_ref, occupancy_ref, tables_ref, green_ref, out_ref, *, where):
    cells = field_ref.shape[-1]
    devices = out_ref.shape[0] // PIECES
    mask = mask_of(occupancy_ref[0], cells)
    table = table_from(tables_ref, where[0:2])
    for part in range(PARTS):
        masked = split(field_ref[part, 0] * mask)
        spread = dot3(table, masked, ((1,), (1,)))
        put_pieces(out_ref, part, spread, devices)

    @pl.when(lax.axis_index("comp") == 1)
    def _():
        pl.delay(BEHIND)


def image_of(part, data_ref, field_ref, inverse_ref, mask, table, devices):
    stack = [
        data_ref[pl.ds((part * PLANES + plane) * 2 + kind, devices, stride=PIECES), :]
        for plane in range(PLANES)
        for kind in range(2)
    ]
    convolved = dot3(table, split(jnp.concatenate(stack, axis=0))).T
    masked = field_ref[part, 0] * mask
    return inverse_ref[0] * masked - mask * convolved


def middle_z_kernel(data_ref, field_ref, inverse_ref, occupancy_ref, tables_ref, image_ref, out_ref, *, where):
    cells = field_ref.shape[-1]
    devices = out_ref.shape[0] // PIECES
    mask = mask_of(occupancy_ref[0], cells)
    table = table_from(tables_ref, where[0:2])
    back = table_from(tables_ref, where[2:4])
    for part in range(PARTS):
        image = image_of(part, data_ref, field_ref, inverse_ref, mask, back, devices)
        image_ref[part, 0] = image
        spread = dot3(table, split(image * mask), ((1,), (1,)))
        put_pieces(out_ref, part, spread, devices)


def last_z_kernel(data_ref, field_ref, inverse_ref, occupancy_ref, tables_ref, image_ref, *, where):
    cells = field_ref.shape[-1]
    devices = data_ref.shape[0] // PIECES
    mask = mask_of(occupancy_ref[0], cells)
    back = table_from(tables_ref, where[2:4])
    for part in range(PARTS):
        image_ref[part, 0] = image_of(part, data_ref, field_ref, inverse_ref, mask, back, devices)


def plane_kernel(data_ref, green_ref, tables_ref, out_ref, spectrum_ref, *, where):
    devices = data_ref.shape[0] // PIECES
    length = green_ref.shape[-1]
    combos = ((0, 3, 4), (3, 1, 5), (4, 5, 2))
    table = table_from(tables_ref, where[4:6])
    table_t = table_from(tables_ref, where[6:8])
    for plane in range(PLANES):

        def piece_of(part, kind):
            return pl.ds((part * PLANES + plane) * 2 + kind, devices, stride=PIECES)

        rows = [
            jnp.concatenate([data_ref[piece_of(part, 0), :], data_ref[piece_of(part, 1), :]], axis=1)
            for part in range(PARTS)
        ]
        along_y = dot3(split(jnp.concatenate(rows, axis=0)), table)
        for part in range(PARTS):
            here = along_y[part * devices : (part + 1) * devices]
            stacked = jnp.concatenate([here[:, :length], here[:, length:]], axis=0)
            spectrum_ref[part] = dot3(table_t, split(stacked))
        rows = []
        for part in range(PARTS):
            row = combos[part]
            first, second, third = green_ref[row[0], plane], green_ref[row[1], plane], green_ref[row[2], plane]

            def product(kind):
                where = slice(kind * length, (kind + 1) * length)
                return (
                    first * spectrum_ref[0, where] + second * spectrum_ref[1, where] + third * spectrum_ref[2, where]
                )

            field = jnp.concatenate([product(0), product(1)], axis=0)
            along_x = dot3(table, split(field))
            rows.append(jnp.concatenate([along_x[:devices], along_x[devices:]], axis=1))
        back = dot3(split(jnp.concatenate(rows, axis=0)), table_t)
        for part in range(PARTS):
            here = back[part * devices : (part + 1) * devices]
            out_ref[piece_of(part, 0), :] = here[:, :devices]
            out_ref[piece_of(part, 1), :] = here[:, devices:]


VMEM = pl.BlockSpec(memory_space=pltpu.VMEM)


def call(kernel, outs, args, flops, scratch=(), mebibytes=12):
    single = not isinstance(outs, tuple)
    moved = sum(a.size * a.dtype.itemsize for a in args)
    return pl.pallas_call(
        kernel,
        out_shape=outs,
        in_specs=[VMEM] * len(args),
        out_specs=VMEM if single else (VMEM,) * len(outs),
        scratch_shapes=list(scratch),
        cost_estimate=pl.CostEstimate(flops=flops, bytes_accessed=moved, transcendentals=0),
        compiler_params=pltpu.CompilerParams(vmem_limit_bytes=mebibytes * 1024 * 1024),
    )(*args)


def exchange(data, devices):
    rows = data.shape[0] // devices
    flat = data.reshape(devices, 1, rows * data.shape[1])
    moved = lax.all_to_all(flat, "slab", split_axis=0, concat_axis=0, tiled=True)
    return moved.reshape(data.shape)


def per_device(devices, polarization, inverse_polarizability, occupancy, green_fourier):
    cells = polarization.shape[-1]
    length = green_fourier.shape[-1]
    packed, where = packed_tables(cells, devices)
    tables = jnp.asarray(packed)
    sent = jax.ShapeDtypeStruct((devices * PIECES, cells), F32)
    image = jax.ShapeDtypeStruct(polarization.shape, F32)
    z_flops = 3 * 2 * PARTS * cells * cells * 2 * length
    plane_flops = 3 * 2 * PARTS * PLANES * (4 * cells * cells * length + 4 * cells * length * length) * 2

    def using(kernel):
        return functools.partial(kernel, where=where)

    def planes_of(data):
        scratch = (pltpu.VMEM((PARTS, 2 * length, length), F32),)
        return call(using(plane_kernel), sent, (data, green_fourier, tables), plane_flops, scratch)

    data = call(using(forward_z_kernel), sent, (polarization, occupancy, tables, green_fourier), z_flops)
    data = exchange(planes_of(exchange(data, devices)), devices)
    first_image, data = call(
        using(middle_z_kernel),
        (image, sent),
        (data, polarization, inverse_polarizability, occupancy, tables),
        2 * z_flops,
    )
    data = exchange(planes_of(exchange(data, devices)), devices)
    second_image = call(
        using(last_z_kernel), image, (data, first_image, inverse_polarizability, occupancy, tables), z_flops
    )
    return (first_image, second_image)


def solution(mesh):
    return jax.shard_map(
        functools.partial(per_device, mesh.shape["slab"]),
        mesh=mesh,
        in_specs=(
            P("comp", "slab", None, None),
            P("slab", None, None),
            P("slab", None, None),
            P(None, "slab", None, None),
        ),
        out_specs=(P("comp", "slab", None, None), P("comp", "slab", None, None)),
        check_vma=False,
    )
```

```python
import functools

import jax
import jax.numpy as jnp
import numpy as np
from jax import lax
from jax.experimental import pallas as pl
from jax.experimental.pallas import tpu as pltpu
from jax.sharding import PartitionSpec as P

BLOCK = 8
LANES = 128
BEHIND = 13000
F32 = jnp.float32
BF16 = jnp.bfloat16
PARTS = 3
PLANES = 2
PIECES = PARTS * PLANES * 2


def halves_of(table):
    high = table.astype(jnp.bfloat16)
    low = (table - high.astype(np.float64)).astype(jnp.bfloat16)
    return (high, low)


def angles(count_in, count_out):
    phase = np.outer(np.arange(count_in), np.arange(count_out)) % count_out
    return 2.0 * np.pi * phase / count_out


def tables_of(cells, devices):
    angle = angles(cells, 2 * cells)
    cosine, sine = np.cos(angle), np.sin(angle)
    plane = np.block([[cosine, -sine], [sine, cosine]])
    both = np.stack([cosine.T, -sine.T]).reshape(2, devices, 2 * cells // devices, cells)
    along_z = both.transpose(2, 0, 1, 3).reshape(4 * cells, cells)
    return (along_z, along_z.T / float((2 * cells) ** 3), plane, plane.T)


def packed_tables(cells, devices):
    blocks, where, row = [], [], 0
    for table in tables_of(cells, devices):
        rows, columns = table.shape
        for half in halves_of(table):
            where.append((row, rows, columns))
            for start in range(0, columns, LANES):
                blocks.append(half[:, start : start + LANES])
                row += rows
    return np.concatenate(blocks, axis=0), where


def table_from(tables_ref, entry):
    def half(row, rows, columns):
        return jnp.concatenate(
            [tables_ref[row + i * rows : row + (i + 1) * rows] for i in range(columns // LANES)], axis=1
        )

    return tuple(half(*one) for one in entry)


def split(value):
    high = value.astype(BF16)
    return (high, (value - high.astype(F32)).astype(BF16))


def dot3(left, right, dims=((1,), (0,))):
    def one(a, b):
        return lax.dot_general(a, b, (dims, ((), ())), preferred_element_type=F32)

    rows = left[0].shape[0]
    both = one(jnp.concatenate(left, axis=0), right[0])
    return both[:rows] + both[rows:] + one(left[0], right[1])


def mask_of(occupancy, cells):
    blocks = occupancy.shape[-1]
    row = lax.broadcasted_iota(jnp.int32, (cells, blocks), 0)
    col = lax.broadcasted_iota(jnp.int32, (cells, blocks), 1)
    expand = jnp.where(row // BLOCK == col, 1.0, 0.0).astype(F32)
    flags = occupancy.astype(F32)
    rows = jnp.dot(expand, flags, preferred_element_type=F32)
    return lax.dot_general(rows, expand, (((1,), (1,)), ((), ())), preferred_element_type=F32)


def put_pieces(out_ref, part, spread, devices):
    for plane in range(PLANES):
        for kind in range(2):
            piece = (part * PLANES + plane) * 2 + kind
            start = (plane * 2 + kind) * devices
            out_ref[pl.ds(piece, devices, stride=PIECES), :] = spread[start : start + devices]


def forward_z_kernel(field_ref, occupancy_ref, tables_ref, green_ref, out_ref, *, where):
    cells = field_ref.shape[-1]
    devices = out_ref.shape[0] // PIECES
    mask = mask_of(occupancy_ref[0], cells)
    table = table_from(tables_ref, where[0:2])
    for part in range(PARTS):
        masked = split(field_ref[part, 0] * mask)
        spread = dot3(table, masked, ((1,), (1,)))
        put_pieces(out_ref, part, spread, devices)

    @pl.when(lax.axis_index("comp") == 1)
    def _():
        pl.delay(BEHIND)


def image_of(part, data_ref, field_ref, inverse_ref, mask, table, devices):
    stack = [
        data_ref[pl.ds((part * PLANES + plane) * 2 + kind, devices, stride=PIECES), :]
        for plane in range(PLANES)
        for kind in range(2)
    ]
    convolved = dot3(table, split(jnp.concatenate(stack, axis=0))).T
    masked = field_ref[part, 0] * mask
    return inverse_ref[0] * masked - mask * convolved


def middle_z_kernel(data_ref, field_ref, inverse_ref, occupancy_ref, tables_ref, image_ref, out_ref, *, where):
    cells = field_ref.shape[-1]
    devices = out_ref.shape[0] // PIECES
    mask = mask_of(occupancy_ref[0], cells)
    table = table_from(tables_ref, where[0:2])
    back = table_from(tables_ref, where[2:4])
    for part in range(PARTS):
        image = image_of(part, data_ref, field_ref, inverse_ref, mask, back, devices)
        image_ref[part, 0] = image
        spread = dot3(table, split(image * mask), ((1,), (1,)))
        put_pieces(out_ref, part, spread, devices)


def last_z_kernel(data_ref, field_ref, inverse_ref, occupancy_ref, tables_ref, image_ref, *, where):
    cells = field_ref.shape[-1]
    devices = data_ref.shape[0] // PIECES
    mask = mask_of(occupancy_ref[0], cells)
    back = table_from(tables_ref, where[2:4])
    for part in range(PARTS):
        image_ref[part, 0] = image_of(part, data_ref, field_ref, inverse_ref, mask, back, devices)


def plane_kernel(data_ref, green_ref, tables_ref, out_ref, spectrum_ref, *, where):
    devices = data_ref.shape[0] // PIECES
    length = green_ref.shape[-1]
    combos = ((0, 3, 4), (3, 1, 5), (4, 5, 2))
    table = table_from(tables_ref, where[4:6])
    table_t = table_from(tables_ref, where[6:8])
    for plane in range(PLANES):

        def piece_of(part, kind):
            return pl.ds((part * PLANES + plane) * 2 + kind, devices, stride=PIECES)

        rows = [
            jnp.concatenate([data_ref[piece_of(part, 0), :], data_ref[piece_of(part, 1), :]], axis=1)
            for part in range(PARTS)
        ]
        along_y = dot3(split(jnp.concatenate(rows, axis=0)), table)
        for part in range(PARTS):
            here = along_y[part * devices : (part + 1) * devices]
            stacked = jnp.concatenate([here[:, :length], here[:, length:]], axis=0)
            spectrum_ref[part] = dot3(table_t, split(stacked))
        rows = []
        for part in range(PARTS):
            row = combos[part]
            first, second, third = green_ref[row[0], plane], green_ref[row[1], plane], green_ref[row[2], plane]

            def product(kind):
                where = slice(kind * length, (kind + 1) * length)
                return (
                    first * spectrum_ref[0, where] + second * spectrum_ref[1, where] + third * spectrum_ref[2, where]
                )

            field = jnp.concatenate([product(0), product(1)], axis=0)
            along_x = dot3(table, split(field))
            rows.append(jnp.concatenate([along_x[:devices], along_x[devices:]], axis=1))
        back = dot3(split(jnp.concatenate(rows, axis=0)), table_t)
        for part in range(PARTS):
            here = back[part * devices : (part + 1) * devices]
            out_ref[piece_of(part, 0), :] = here[:, :devices]
            out_ref[piece_of(part, 1), :] = here[:, devices:]


VMEM = pl.BlockSpec(memory_space=pltpu.VMEM)


def call(kernel, outs, args, flops, scratch=(), mebibytes=12):
    single = not isinstance(outs, tuple)
    moved = sum(a.size * a.dtype.itemsize for a in args)
    return pl.pallas_call(
        kernel,
        out_shape=outs,
        in_specs=[VMEM] * len(args),
        out_specs=VMEM if single else (VMEM,) * len(outs),
        scratch_shapes=list(scratch),
        cost_estimate=pl.CostEstimate(flops=flops, bytes_accessed=moved, transcendentals=0),
        compiler_params=pltpu.CompilerParams(vmem_limit_bytes=mebibytes * 1024 * 1024),
    )(*args)


def exchange(data, devices):
    rows = data.shape[0] // devices
    flat = data.reshape(devices, 1, rows * data.shape[1])
    moved = lax.all_to_all(flat, "slab", split_axis=0, concat_axis=0, tiled=True)
    return moved.reshape(data.shape)


def per_device(devices, polarization, inverse_polarizability, occupancy, green_fourier):
    cells = polarization.shape[-1]
    length = green_fourier.shape[-1]
    packed, where = packed_tables(cells, devices)
    tables = jnp.asarray(packed)
    sent = jax.ShapeDtypeStruct((devices * PIECES, cells), F32)
    image = jax.ShapeDtypeStruct(polarization.shape, F32)
    z_flops = 3 * 2 * PARTS * cells * cells * 2 * length
    plane_flops = 3 * 2 * PARTS * PLANES * (4 * cells * cells * length + 4 * cells * length * length) * 2

    def using(kernel):
        return functools.partial(kernel, where=where)

    def planes_of(data):
        scratch = (pltpu.VMEM((PARTS, 2 * length, length), F32),)
        return call(using(plane_kernel), sent, (data, green_fourier, tables), plane_flops, scratch)

    data = call(using(forward_z_kernel), sent, (polarization, occupancy, tables, green_fourier), z_flops)
    data = exchange(planes_of(exchange(data, devices)), devices)
    first_image, data = call(
        using(middle_z_kernel),
        (image, sent),
        (data, polarization, inverse_polarizability, occupancy, tables),
        2 * z_flops,
    )
    data = exchange(planes_of(exchange(data, devices)), devices)
    second_image = call(
        using(last_z_kernel), image, (data, first_image, inverse_polarizability, occupancy, tables), z_flops
    )
    return (first_image, second_image)


def solution(mesh):
    return jax.shard_map(
        functools.partial(per_device, mesh.shape["slab"]),
        mesh=mesh,
        in_specs=(
            P("comp", "slab", None, None),
            P("slab", None, None),
            P("slab", None, None),
            P(None, "slab", None, None),
        ),
        out_specs=(P("comp", "slab", None, None), P("comp", "slab", None, None)),
        check_vma=False,
    )
```
